32 devices in a mesh: seq: 16 (over z, y, x), head: 2 (over core).
Axes of the slice: x: 2, y: 2, z: 4, core: 2. Of those that a mesh axis runs over, the one named last changes fastest.
Arguments:
- queries: bfloat16 [3072, 32, 128], P('seq', 'head'), may hold values from -180 to 180
- key_rows: bfloat16 [3072, 8, 128], P('seq', 'head'), may hold values from -4.5 to 4.5
- value_rows: bfloat16 [3072, 8, 128], P('seq', 'head'), may hold values from -24 to 24
- windows: int32 [32], P('head'), may hold values from 768 to 1536, as said below
- sink_counts: int32 [32], P('head'), may hold values from 1 to 4, as said below
- sink_bias: float32 [32], P('head'), may hold values from 3 to 7
- out_weight: bfloat16 [4096, 4096], P('head'), may hold values from -0.09375 to 0.09375
Outputs:
- attn_out: bfloat16 [3072, 4096], P(('seq', 'head'))
The draws below stay inside these ranges and needn't reach their ends.
Inputs may be any that keep to these rules, and one draw needn't show every extreme that they name: `windows`: each head's window lies between 768 and 1536, and some head has exactly 1536. `sink_counts`: each head has 1 to 4 sink tokens, and some head has exactly 4.
All inputs are finite; a program needn't handle non-finite values.
Results may differ from the reference program's by a relative error of at most 0.018.
Values may be sent and summed in bfloat16 or wider, within the bound.
A program may use at most 128 MiB of HBM per device.

```python
import jax
import jax.numpy as jnp
from jax import lax

D = 4096
H = 32
KVH = 8
HD = 128
WINDOW = 1536
SINKS = 4
TOK_DEV = 192
TOKENS = 3072
N_SEQ = 16
N_HEAD = 2


def shared_keys(key):
    return jnp.clip(jax.random.normal(jax.random.fold_in(key, 11), (TOKENS, KVH, HD), jnp.float32), -4.5, 4.5)


def draw_key_rows(key, part):
    return shared_keys(key).astype(jnp.bfloat16)


def draw_queries(key, part):
    base = jnp.clip(jax.random.normal(jax.random.fold_in(key, 12), (TOKENS, H, HD), jnp.float32), -4.5, 4.5)
    return base.astype(jnp.bfloat16)


def draw_windows(key, part):
    spread = jax.random.randint(jax.random.fold_in(key, 21), (H,), WINDOW // 2, WINDOW + 1)
    chosen = jax.random.randint(jax.random.fold_in(key, 22), (), 0, H)
    return jnp.where(jnp.arange(H) == chosen, WINDOW, spread).astype(jnp.int32)


def draw_sink_counts(key, part):
    spread = jax.random.randint(jax.random.fold_in(key, 31), (H,), 1, SINKS + 1)
    chosen = jax.random.randint(jax.random.fold_in(key, 32), (), 0, H)
    return jnp.where(jnp.arange(H) == chosen, SINKS, spread).astype(jnp.int32)


def steps_of(stream_key, dims, split, least, high):
    def one(dim, blocks):
        draws = jax.random.uniform(jax.random.fold_in(jax.random.fold_in(stream_key, 6), dim), (blocks,), jnp.float32, least / len(split), high / len(split))
        return jnp.repeat(jnp.exp(draws), dims[dim] // blocks).reshape((-1,) + (1,) * (len(dims) - dim - 1))

    level = one(*split[0])
    for cut in split[1:]:
        level = level * one(*cut)
    return level


def noise(own_key, extent, scale, most, pieces=(), held_as=jnp.bfloat16):
    values = jax.random.normal(own_key, extent, jnp.float32) * scale
    if len(pieces) > 0:
        values = steps_of(own_key, extent, pieces, -0.22, 0.18) * values
    return jnp.clip(values, min=-most, max=most).astype(held_as)


def setup_inputs(seed: int = 0) -> dict:
    streams_of = jax.random.split(jax.random.key(seed), 8)
    return {
        "queries": draw_queries(jax.random.fold_in(streams_of[7], 71), 0),
        "key_rows": draw_key_rows(jax.random.fold_in(streams_of[7], 71), 0),
        "value_rows": noise(streams_of[2], (TOKENS, KVH, HD), 4.0, 24.0, ((0, 16), (1, 2))),
        "windows": draw_windows(jax.random.fold_in(streams_of[7], 71), 0),
        "sink_counts": draw_sink_counts(jax.random.fold_in(streams_of[7], 71), 0),
        "sink_bias": jnp.clip(3.0 + 4.0 * jax.random.uniform(streams_of[5], (H,), jnp.float32) ** steps_of(streams_of[5], (H,), ((0, 2),), -0.2, 0.2), 3.0, 7.0),
        "out_weight": noise(streams_of[6], (H * HD, D), (H * HD) ** -0.5, 0.09375, ((0, 2),)),
    }


def attend_block(query_block, band_rows, sink_rows, first_pos, windows, sink_counts, sink_bias):
    tok_rows, local_heads, head_width = query_block.shape
    kv_local = band_rows.shape[2]
    group_size = local_heads // kv_local
    band_span = band_rows.shape[1]
    all_keys = jnp.concatenate([sink_rows[0], band_rows[0]], axis=0)
    all_values = jnp.concatenate([sink_rows[1], band_rows[1]], axis=0)
    grouped = query_block.reshape(tok_rows, kv_local, group_size, head_width)
    score_scale = 1.0 / (head_width ** 0.5)
    scores = jnp.einsum("tkgd,skd->kgts", grouped.astype(jnp.float32), all_keys.astype(jnp.float32)) * score_scale
    query_pos = first_pos + jnp.arange(tok_rows, dtype=jnp.int32)
    band_pos = first_pos + tok_rows - band_span + jnp.arange(band_span, dtype=jnp.int32)
    sink_pos = jnp.arange(SINKS, dtype=jnp.int32)
    key_pos = jnp.concatenate([sink_pos, band_pos])
    is_sink = jnp.concatenate([jnp.ones((SINKS,), bool), jnp.zeros((band_span,), bool)])
    head_window = windows.reshape(kv_local, group_size, 1, 1)
    head_sinks = sink_counts.reshape(kv_local, group_size, 1, 1)
    head_bias = sink_bias.reshape(kv_local, group_size, 1, 1)
    distance = query_pos[:, None] - key_pos[None, :]
    visible = (distance >= 0) & jnp.where(is_sink, key_pos < head_sinks, (distance < head_window) & (key_pos >= head_sinks))
    scores = scores + jnp.where(is_sink, head_bias, 0.0)
    masked = jnp.where(visible, scores, -1e30)
    highest = jnp.max(masked, axis=-1, keepdims=True)
    weights = jnp.where(visible, jnp.exp(masked - highest), 0.0)
    normed = (weights / jnp.sum(weights, axis=-1, keepdims=True)).astype(jnp.bfloat16)
    mixed = jnp.einsum("kgts,skd->tkgd", normed.astype(jnp.float32), all_values.astype(jnp.float32))
    return mixed.astype(jnp.bfloat16).reshape(tok_rows, local_heads * head_width)


def reference(queries, key_rows, value_rows, windows, sink_counts, sink_bias, out_weight):
    stacked = jnp.stack([key_rows, value_rows])
    padding = jnp.zeros((2, WINDOW, KVH, HD), jnp.bfloat16)
    padded = jnp.concatenate([padding, stacked], axis=1)
    sink_rows = stacked[:, :SINKS]

    def one_shard(shard_index):
        first_pos = (shard_index * TOK_DEV).astype(jnp.int32)
        query_block = lax.dynamic_slice_in_dim(queries, first_pos, TOK_DEV, 0)
        band_rows = lax.dynamic_slice_in_dim(padded, first_pos, TOK_DEV + WINDOW, 1)
        return attend_block(query_block, band_rows, sink_rows, first_pos, windows, sink_counts, sink_bias)

    attended = lax.map(one_shard, jnp.arange(N_SEQ, dtype=jnp.int32)).reshape(TOKENS, H * HD)
    group_rows = H * HD // N_HEAD
    total = jnp.zeros((TOKENS, D), jnp.float32)
    for member in range(N_HEAD):
        lower = member * group_rows
        term = jnp.dot(attended[:, lower:lower + group_rows], out_weight[lower:lower + group_rows], preferred_element_type=jnp.float32)
        total = total + lax.optimization_barrier(term.astype(jnp.bfloat16)).astype(jnp.float32)
    return total.astype(jnp.bfloat16)
```

```python
import functools

import jax
import jax.numpy as jnp
from jax import lax
from jax.experimental import pallas as pl
from jax.experimental.pallas import tpu as pltpu
from jax.sharding import PartitionSpec as P

WINDOW = 1536
SINKS = 4
PLANE = 4
SINK_ROWS = 16
HIDDEN = -1e30
LOG2E = 1.4426950408889634
MESH = pl.DeviceIdType.MESH


def kernel(
    n_seq, n_head, tile,
    win_ref, cnt_ref, bias_ref, own, q_ref, w_hbm, out_ref,
    kv, sink, qt, low, few, lift, top, norm, acc, att, w, part, got,
    send_sem, recv_sem, sink_send, sink_recv, w_sem, part_send, part_recv,
):
    me, side = lax.axis_index("seq"), lax.axis_index("head")
    heads_kv, _, rows, width = own.shape
    lanes = q_ref.shape[1]
    group = lanes // rows
    model = w.shape[1]
    share = rows // n_head
    z, p = me // PLANE, lax.rem(me, PLANE)
    bit0, bit1 = lax.rem(p, 2), p // 2
    px, py = p + 1 - 2 * bit0, p + 2 - 4 * bit1
    pd = 3 - p
    base = z * PLANE
    n_z = n_seq // PLANE
    scale = LOG2E / width**0.5

    barrier = pltpu.get_barrier_semaphore()

    def greet(axis, here, count):
        def one(step, carry):
            pl.semaphore_signal(
                barrier, inc=1, device_id={axis: lax.rem(here + step, count)}, device_id_type=MESH
            )
            return carry
        lax.fori_loop(1, count, one, 0)

    greet("seq", me, n_seq)
    greet("head", side, n_head)
    pl.semaphore_wait(barrier, n_seq + n_head - 2)

    def send(kind, src, plane, source, c, target):
        return pltpu.make_async_remote_copy(
            src_ref=src,
            dst_ref=kv.at[plane * PLANE + source, c],
            send_sem=send_sem.at[kind, c],
            recv_sem=recv_sem.at[plane * PLANE + source, c],
            device_id={"seq": target},
            device_id_type=MESH,
        )

    def landed(plane, source, c):
        send(0, own.at[c], plane, source, c, me).wait_recv()

    def held(plane, source, c):
        return kv.at[plane * PLANE + source, c]

    x_old, y_old, d_old = 2 * bit0, 2 * bit1, 2 * bit1
    x_from, y_from, d_from = 2 - 2 * bit0, 2 - 2 * bit1, 2 - 2 * bit1

    def sink_copy(target):
        return pltpu.make_async_remote_copy(
            src_ref=own.at[:, :, pl.ds(0, SINK_ROWS)],
            dst_ref=sink,
            send_sem=sink_send.at[target],
            recv_sem=sink_recv,
            device_id={"seq": target},
            device_id_type=MESH,
        )

    for c in range(heads_kv):
        @pl.when(z + 1 < n_z)
        def _():
            send(0, own.at[c], 1, p, c, me + PLANE).start()

        @pl.when(x_old == 0)
        def _():
            send(2, own.at[c], 0, p, c, base + px).start()

        @pl.when(y_old == 0)
        def _():
            send(3, own.at[c], 0, p, c, base + py).start()

        if c == 0:
            @pl.when(me == 0)
            def _():
                def one(target, carry):
                    sink_copy(target).start()
                    return carry
                lax.fori_loop(1, n_seq, one, 0)

    fetch = pltpu.make_async_copy(w_hbm, w, w_sem)
    fetch.start()

    column = lax.broadcasted_iota(jnp.int32, (1, lanes), 1)
    for c in range(heads_kv):
        window, count, bias, token = (jnp.zeros((1, lanes), t) for t in (jnp.int32, jnp.int32, jnp.float32, jnp.int32))
        for g in range(group):
            mine = (column >= g * rows) & (column < (g + 1) * rows)
            h = c * group + g
            window = jnp.where(mine, win_ref[h], window)
            count = jnp.where(mine, cnt_ref[h], count)
            bias = jnp.where(mine, bias_ref[h], bias)
            token = jnp.where(mine, column - g * rows, token)
        token = token + me * rows
        low[c] = jnp.maximum(token - window, count - 1)
        few[c] = jnp.minimum(token, count - 1)
        lift[c] = bias * LOG2E
        qt[c] = q_ref[c].T
        top[c] = jnp.full((1, lanes), HIDDEN, jnp.float32)
        norm[c] = jnp.zeros((1, lanes), jnp.float32)
        acc[c] = jnp.zeros((width, lanes), jnp.float32)

    def attend(block, c, shard, causal=False, sinks=False):
        keys, values = block[0], block[1]
        key_row = lax.broadcasted_iota(jnp.int32, (keys.shape[0], 1), 0)
        for n in range(0, lanes, 256):
            cols = slice(n, n + 256)
            s = jnp.dot(keys, qt[c, :, cols], preferred_element_type=jnp.float32) * scale
            if sinks:
                s = jnp.where(key_row <= few[c, :, cols], s + lift[c, :, cols], HIDDEN)
            else:
                seen = key_row > low[c, :, cols] - shard * rows
                if causal:
                    token = lax.rem(lax.broadcasted_iota(jnp.int32, (1, 256), 1) + n, rows)
                    seen = seen & (key_row <= token)
                s = jnp.where(seen, s, HIDDEN)
            old = top[c, :, cols]
            new = jnp.maximum(old, jnp.max(s, axis=0, keepdims=True))
            e = jnp.exp2(s - new)
            fade = jnp.exp2(old - new)
            top[c, :, cols] = new
            norm[c, :, cols] = norm[c, :, cols] * fade + jnp.sum(e, axis=0, keepdims=True)
            acc[c, :, cols] = acc[c, :, cols] * fade + lax.dot_general(
                values, e.astype(jnp.bfloat16), (((0,), (0,)), ((), ())),
                preferred_element_type=jnp.float32,
            )

    def each(body):
        def one(c, carry):
            body(c)
            return carry
        lax.fori_loop(0, heads_kv, one, 0)

    each(lambda c: attend(own.at[c], c, me, causal=True))

    @pl.when(z >= 1)
    def _():
        def first(c):
            landed(1, p, c)

            @pl.when(z + 1 < n_z)
            def _():
                send(1, held(1, p, c), 2, p, c, me + PLANE).start()

            send(4, held(1, p, c), 1, p, c, base + px).start()
            send(5, held(1, p, c), 1, p, c, base + py).start()
            attend(held(1, p, c), c, me - PLANE)
        each(first)

        def second(c):
            @pl.when(z >= 2)
            def _():
                landed(2, p, c)

                @pl.when(x_old == 2)
                def _():
                    send(2, held(2, p, c), 2, p, c, base + px).start()

                @pl.when(y_old == 2)
                def _():
                    send(3, held(2, p, c), 2, p, c, base + py).start()

            landed(1, px, c)
            send(6, held(1, px, c), 1, px, c, base + py).start()
            attend(held(1, px, c), c, base - PLANE + px)
        each(second)

    def relay(c):
        @pl.when(z >= y_from)
        def _():
            landed(y_from, py, c)
            send(7, held(y_from, py, c), y_from, py, c, base + px).start()
            attend(held(y_from, py, c), c, base - y_from * PLANE + py)
    each(relay)

    @pl.when(me == 0)
    def _():
        each(lambda c: attend(own.at[c, :, pl.ds(0, SINK_ROWS)], c, 0, sinks=True))

    @pl.when(me > 0)
    def _():
        sink_copy(me).wait_recv()
        each(lambda c: attend(sink.at[c], c, 0, sinks=True))

    @pl.when(z >= 2)
    def _():
        each(lambda c: attend(held(2, p, c), c, me - 2 * PLANE))

    @pl.when(z >= 1)
    def _():
        def third(c):
            landed(1, py, c)
            attend(held(1, py, c), c, base - PLANE + py)
        each(third)

    @pl.when(z >= x_from)
    def _():
        def fourth(c):
            landed(x_from, px, c)
            attend(held(x_from, px, c), c, base - x_from * PLANE + px)
        each(fourth)

    @pl.when(z >= 1)
    def _():
        def fifth(c):
            landed(1, pd, c)
            attend(held(1, pd, c), c, base - PLANE + pd)
        each(fifth)

    @pl.when(z >= d_from)
    def _():
        def sixth(c):
            landed(d_from, pd, c)
            attend(held(d_from, pd, c), c, base - d_from * PLANE + pd)
        each(sixth)

    for c in range(heads_kv):
        mixed = (acc[c] / norm[c]).T.astype(jnp.bfloat16)
        for g in range(group):
            h = c * group + g
            att[:, h * width:(h + 1) * width] = mixed[g * rows:(g + 1) * rows]

    fetch.wait()
    tiles = model // tile

    def give(t, step):
        target = lax.rem(side + step, n_head)
        return pltpu.make_async_remote_copy(
            src_ref=part.at[t, target],
            dst_ref=got.at[t, step - 1],
            send_sem=part_send.at[t, step - 1],
            recv_sem=part_recv.at[t, step - 1],
            device_id={"head": target},
            device_id_type=MESH,
        )

    def project(t, carry):
        cols = pl.ds(pl.multiple_of(t * tile, tile), tile)
        total = jnp.dot(att[...], w[:, cols], preferred_element_type=jnp.float32)
        for d in range(n_head):
            part[t, d] = total[d * share:(d + 1) * share].astype(jnp.bfloat16)

        @pl.when(t >= 1)
        def _():
            for step in range(1, n_head):
                give(t - 1, step).start()
        return carry
    lax.fori_loop(0, tiles, project, 0)
    for step in range(1, n_head):
        give(tiles - 1, step).start()

    def finish(t, carry):
        total = part[t, side].astype(jnp.float32)
        for step in range(1, n_head):
            give(t, step).wait_recv()
            total = total + got[t, step - 1].astype(jnp.float32)
        out_ref[:, pl.ds(pl.multiple_of(t * tile, tile), tile)] = total.astype(jnp.bfloat16)
        return carry
    lax.fori_loop(0, tiles, finish, 0)

    def sent(kind, plane, source, c, target):
        send(kind, held(plane, source, c), plane, source, c, target).wait_send()

    def drain(c):
        @pl.when(z + 1 < n_z)
        def _():
            sent(0, 1, p, c, me + PLANE)

        @pl.when(z >= x_old)
        def _():
            sent(2, x_old, p, c, base + px)

        @pl.when(z >= y_old)
        def _():
            sent(3, y_old, p, c, base + py)

        @pl.when(z >= 1)
        def _():
            @pl.when(z + 1 < n_z)
            def _():
                sent(1, 2, p, c, me + PLANE)
            sent(4, 1, p, c, base + px)
            sent(5, 1, p, c, base + py)
            sent(6, 1, px, c, base + py)

        @pl.when(z >= y_from)
        def _():
            sent(7, y_from, py, c, base + px)
    each(drain)

    @pl.when(me == 0)
    def _():
        def one(target, carry):
            sink_copy(target).wait_send()
            return carry
        lax.fori_loop(1, n_seq, one, 0)

    def gone(t, carry):
        for step in range(1, n_head):
            give(t, step).wait_send()
        return carry
    lax.fori_loop(0, tiles, gone, 0)


def shards(n_seq, n_head, queries, key_rows, value_rows, windows, sink_counts, sink_bias, out_weight):
    rows, heads, width = queries.shape
    kv_heads = key_rows.shape[1]
    group = heads // kv_heads
    lanes = group * rows
    depth, model = out_weight.shape
    assert (WINDOW - 1) // rows + 1 == 2 * PLANE and n_seq % PLANE == 0
    own = jnp.stack([key_rows, value_rows]).transpose(2, 0, 1, 3)
    q = queries.transpose(1, 0, 2).reshape(kv_heads, lanes, width)
    tile = min(512, model)
    tiles = model // tile
    share = rows // n_head
    bf16, f32, i32 = jnp.bfloat16, jnp.float32, jnp.int32
    vmem = pl.BlockSpec(memory_space=pltpu.VMEM)
    smem = pl.BlockSpec(memory_space=pltpu.SMEM)
    dma = pltpu.SemaphoreType.DMA
    return pl.pallas_call(
        functools.partial(kernel, n_seq, n_head, tile),
        out_shape=jax.ShapeDtypeStruct((share, model), bf16),
        in_specs=[smem, smem, smem, vmem, vmem, pl.BlockSpec(memory_space=pl.ANY)],
        out_specs=vmem,
        scratch_shapes=[
            pltpu.VMEM((3 * PLANE, kv_heads, 2, rows, width), bf16),
            pltpu.VMEM((kv_heads, 2, SINK_ROWS, width), bf16),
            pltpu.VMEM((kv_heads, width, lanes), bf16),
            pltpu.VMEM((kv_heads, 1, lanes), i32),
            pltpu.VMEM((kv_heads, 1, lanes), i32),
            pltpu.VMEM((kv_heads, 1, lanes), f32),
            pltpu.VMEM((kv_heads, 1, lanes), f32),
            pltpu.VMEM((kv_heads, 1, lanes), f32),
            pltpu.VMEM((kv_heads, width, lanes), f32),
            pltpu.VMEM((rows, depth), bf16),
            pltpu.VMEM((depth, model), bf16),
            pltpu.VMEM((tiles, n_head, share, tile), bf16),
            pltpu.VMEM((tiles, n_head - 1, share, tile), bf16),
            dma((8, kv_heads)),
            dma((3 * PLANE, kv_heads)),
            dma((n_seq,)),
            dma,
            dma,
            dma((tiles, n_head - 1)),
            dma((tiles, n_head - 1)),
        ],
        compiler_params=pltpu.CompilerParams(
            collective_id=0, has_side_effects=True, vmem_limit_bytes=56 * 1024 * 1024
        ),
    )(windows, sink_counts, sink_bias, own, q, out_weight)


def solution(mesh):
    in_specs = (
        P("seq", "head", None),
        P("seq", "head", None),
        P("seq", "head", None),
        P("head"),
        P("head"),
        P("head"),
        P("head", None),
    )
    body = functools.partial(shards, mesh.shape["seq"], mesh.shape["head"])
    out_specs = P(("seq", "head"), None)
    return jax.shard_map(body, mesh=mesh, in_specs=in_specs, out_specs=out_specs, check_vma=False)
```

```python
import functools

import jax
import jax.numpy as jnp
from jax import lax
from jax.experimental import pallas as pl
from jax.experimental.pallas import tpu as pltpu
from jax.sharding import PartitionSpec as P

WINDOW = 1536
SINKS = 4
PLANE = 4
SINK_ROWS = 16
HIDDEN = -1e30
LOG2E = 1.4426950408889634
MESH = pl.DeviceIdType.MESH


def kernel(
    n_seq, n_head, tile,
    win_ref, cnt_ref, bias_ref, k_hbm, v_hbm, q_hbm, w_hbm, out_ref,
    own, q_ref, kv, sink, qt, low, few, lift, top, norm, acc, att, w, part, got,
    send_sem, recv_sem, sink_send, sink_recv, own_sem, q_sem, w_sem, part_send, part_recv,
):
    me, side = lax.axis_index("seq"), lax.axis_index("head")
    heads_kv, _, rows, width = own.shape
    lanes = q_ref.shape[1]
    group = lanes // rows
    model = w.shape[1]
    share = rows // n_head
    z, p = me // PLANE, lax.rem(me, PLANE)
    bit0, bit1 = lax.rem(p, 2), p // 2
    px, py = p + 1 - 2 * bit0, p + 2 - 4 * bit1
    pd = 3 - p
    base = z * PLANE
    n_z = n_seq // PLANE
    scale = LOG2E / width**0.5

    barrier = pltpu.get_barrier_semaphore()

    def greet(where):
        pl.semaphore_signal(barrier, inc=1, device_id=where, device_id_type=MESH)

    above, below = (z + 1 < n_z).astype(jnp.int32), (z > 0).astype(jnp.int32)
    loads = [
        pltpu.make_async_copy(ref.at[c], own.at[c, k], own_sem.at[c, k])
        for c in range(heads_kv) for k, ref in enumerate((k_hbm, v_hbm))
    ]
    for load in loads:
        load.start()
    q_load = pltpu.make_async_copy(q_hbm, q_ref, q_sem)
    q_load.start()
    greet({"seq": base + px})
    greet({"seq": base + py})

    @pl.when(z + 1 < n_z)
    def _():
        greet({"seq": me + PLANE})

    @pl.when(z > 0)
    def _():
        greet({"seq": me - PLANE})

    for step in range(1, n_head):
        greet({"head": lax.rem(side + step, n_head)})
    pl.semaphore_wait(barrier, n_head + 1 + above + below)

    def send(kind, src, plane, source, c, target):
        return pltpu.make_async_remote_copy(
            src_ref=src,
            dst_ref=kv.at[plane * PLANE + source, c],
            send_sem=send_sem.at[kind, c],
            recv_sem=recv_sem.at[plane * PLANE + source, c],
            device_id={"seq": target},
            device_id_type=MESH,
        )

    def landed(plane, source, c):
        send(0, own.at[c], plane, source, c, me).wait_recv()

    def held(plane, source, c):
        return kv.at[plane * PLANE + source, c]

    x_old, y_old, d_old = 2 * bit0, 2 * bit1, 2 * bit1
    x_from, y_from, d_from = 2 - 2 * bit0, 2 - 2 * bit1, 2 - 2 * bit1

    def sink_copy(way, source, target):
        return pltpu.make_async_remote_copy(
            src_ref=source,
            dst_ref=sink,
            send_sem=sink_send.at[way],
            recv_sem=sink_recv,
            device_id={"seq": target},
            device_id_type=MESH,
        )

    first_rows = own.at[:, :, pl.ds(0, SINK_ROWS)]

    for load in loads:
        load.wait()
    for c in range(heads_kv):
        @pl.when(z + 1 < n_z)
        def _():
            send(0, own.at[c], 1, p, c, me + PLANE).start()

        @pl.when(x_old == 0)
        def _():
            send(2, own.at[c], 0, p, c, base + px).start()

        @pl.when(y_old == 0)
        def _():
            send(3, own.at[c], 0, p, c, base + py).start()

        if c == 0:
            @pl.when(me == 0)
            def _():
                sink_copy(0, first_rows, base + px).start()
                sink_copy(1, first_rows, base + py).start()

                @pl.when(z + 1 < n_z)
                def _():
                    sink_copy(2, first_rows, me + PLANE).start()

    fetch = pltpu.make_async_copy(w_hbm, w, w_sem)
    fetch.start()

    q_load.wait()
    column = lax.broadcasted_iota(jnp.int32, (1, lanes), 1)
    for c in range(heads_kv):
        window, count, bias, token = (jnp.zeros((1, lanes), t) for t in (jnp.int32, jnp.int32, jnp.float32, jnp.int32))
        for g in range(group):
            mine = (column >= g * rows) & (column < (g + 1) * rows)
            h = c * group + g
            window = jnp.where(mine, win_ref[h], window)
            count = jnp.where(mine, cnt_ref[h], count)
            bias = jnp.where(mine, bias_ref[h], bias)
            token = jnp.where(mine, column - g * rows, token)
        token = token + me * rows
        low[c] = jnp.maximum(token - window, count - 1)
        few[c] = jnp.minimum(token, count - 1)
        lift[c] = bias * LOG2E
        qt[c] = q_ref[c].T
        top[c] = jnp.full((1, lanes), HIDDEN, jnp.float32)
        norm[c] = jnp.zeros((1, lanes), jnp.float32)
        acc[c] = jnp.zeros((width, lanes), jnp.float32)

    def attend(block, c, shard, causal=False, sinks=False):
        keys, values = block[0], block[1]
        key_row = lax.broadcasted_iota(jnp.int32, (keys.shape[0], 1), 0)
        step = min(256, lanes)
        parts = [slice(n, n + step) for n in range(0, lanes, step)]
        scores = [jnp.dot(keys, qt[c, :, cols], preferred_element_type=jnp.float32) for cols in parts]
        turned = values.T
        olds = [top[c, :, cols] for cols in parts]
        weights, news, fades, sums = [], [], [], []
        for s, old, cols in zip(scores, olds, parts):
            s = s * scale
            if sinks:
                s = jnp.where(key_row <= few[c, :, cols], s + lift[c, :, cols], HIDDEN)
            else:
                seen = key_row > low[c, :, cols] - shard * rows
                if causal:
                    column = lax.broadcasted_iota(jnp.int32, (1, step), 1) + cols.start
                    seen = seen & (key_row <= lax.rem(column, rows))
                s = jnp.where(seen, s, HIDDEN)
            new = jnp.maximum(old, jnp.max(s, axis=0, keepdims=True))
            e = jnp.exp2(s - new)
            weights.append(e.astype(jnp.bfloat16))
            news.append(new)
            fades.append(jnp.exp2(old - new))
            sums.append(jnp.sum(e, axis=0, keepdims=True))
        adds = [jnp.dot(turned, e, preferred_element_type=jnp.float32) for e in weights]
        for new, fade, total, add, cols in zip(news, fades, sums, adds, parts):
            top[c, :, cols] = new
            norm[c, :, cols] = norm[c, :, cols] * fade + total
            acc[c, :, cols] = acc[c, :, cols] * fade + add

    def each(body):
        def one(c, carry):
            body(c)
            return carry
        lax.fori_loop(0, heads_kv, one, 0)

    each(lambda c: attend(own.at[c], c, me, causal=True))

    @pl.when(z >= 1)
    def _():
        def first(c):
            landed(1, p, c)

            @pl.when(z + 1 < n_z)
            def _():
                send(1, held(1, p, c), 2, p, c, me + PLANE).start()

            send(4, held(1, p, c), 1, p, c, base + px).start()
            send(5, held(1, p, c), 1, p, c, base + py).start()
            attend(held(1, p, c), c, me - PLANE)
        each(first)

    def pass_on():
        sink_copy(0, sink, me).wait_recv()

        @pl.when(me == 1)
        def _():
            sink_copy(1, sink, base + py).start()

        @pl.when(z + 1 < n_z)
        def _():
            sink_copy(2, sink, me + PLANE).start()

    @pl.when((me > 0) & (z <= 1))
    def _():
        pass_on()

    @pl.when(z >= 1)
    def _():
        def second(c):
            @pl.when(z >= 2)
            def _():
                landed(2, p, c)

                @pl.when(x_old == 2)
                def _():
                    send(2, held(2, p, c), 2, p, c, base + px).start()

                @pl.when(y_old == 2)
                def _():
                    send(3, held(2, p, c), 2, p, c, base + py).start()

            landed(1, px, c)
            send(6, held(1, px, c), 1, px, c, base + py).start()
            attend(held(1, px, c), c, base - PLANE + px)
        each(second)

    def relay(c):
        @pl.when(z >= y_from)
        def _():
            landed(y_from, py, c)
            send(7, held(y_from, py, c), y_from, py, c, base + px).start()
            attend(held(y_from, py, c), c, base - y_from * PLANE + py)
    each(relay)

    @pl.when(z >= 2)
    def _():
        pass_on()

    @pl.when(me == 0)
    def _():
        each(lambda c: attend(own.at[c, :, pl.ds(0, SINK_ROWS)], c, 0, sinks=True))

    @pl.when(me > 0)
    def _():
        each(lambda c: attend(sink.at[c], c, 0, sinks=True))

    @pl.when(z >= 2)
    def _():
        each(lambda c: attend(held(2, p, c), c, me - 2 * PLANE))

    @pl.when(z >= 1)
    def _():
        def third(c):
            landed(1, py, c)
            attend(held(1, py, c), c, base - PLANE + py)
        each(third)

    @pl.when(z >= x_from)
    def _():
        def fourth(c):
            landed(x_from, px, c)
            attend(held(x_from, px, c), c, base - x_from * PLANE + px)
        each(fourth)

    @pl.when(z >= 1)
    def _():
        def fifth(c):
            landed(1, pd, c)
            attend(held(1, pd, c), c, base - PLANE + pd)
        each(fifth)

    @pl.when(z >= d_from)
    def _():
        def sixth(c):
            landed(d_from, pd, c)
            attend(held(d_from, pd, c), c, base - d_from * PLANE + pd)
        each(sixth)

    for c in range(heads_kv):
        mixed = (acc[c] / norm[c]).T.astype(jnp.bfloat16)
        for g in range(group):
            h = c * group + g
            att[:, h * width:(h + 1) * width] = mixed[g * rows:(g + 1) * rows]

    fetch.wait()
    tiles = model // tile

    def give(t, step):
        target = lax.rem(side + step, n_head)
        return pltpu.make_async_remote_copy(
            src_ref=part.at[t, target],
            dst_ref=got.at[t, step - 1],
            send_sem=part_send.at[t, step - 1],
            recv_sem=part_recv.at[t, step - 1],
            device_id={"head": target},
            device_id_type=MESH,
        )

    def project(t, carry):
        cols = pl.ds(pl.multiple_of(t * tile, tile), tile)
        total = jnp.dot(att[...], w[:, cols], preferred_element_type=jnp.float32)
        for d in range(n_head):
            part[t, d] = total[d * share:(d + 1) * share].astype(jnp.bfloat16)

        @pl.when(t >= 1)
        def _():
            for step in range(1, n_head):
                give(t - 1, step).start()
        return carry
    lax.fori_loop(0, tiles, project, 0)
    for step in range(1, n_head):
        give(tiles - 1, step).start()

    def finish(t, carry):
        total = part[t, side].astype(jnp.float32)
        for step in range(1, n_head):
            give(t, step).wait_recv()
            total = total + got[t, step - 1].astype(jnp.float32)
        out_ref[:, pl.ds(pl.multiple_of(t * tile, tile), tile)] = total.astype(jnp.bfloat16)
        return carry
    lax.fori_loop(0, tiles, finish, 0)

    def sent(kind, plane, source, c, target):
        send(kind, held(plane, source, c), plane, source, c, target).wait_send()

    def drain(c):
        @pl.when(z + 1 < n_z)
        def _():
            sent(0, 1, p, c, me + PLANE)

        @pl.when(z >= x_old)
        def _():
            sent(2, x_old, p, c, base + px)

        @pl.when(z >= y_old)
        def _():
            sent(3, y_old, p, c, base + py)

        @pl.when(z >= 1)
        def _():
            @pl.when(z + 1 < n_z)
            def _():
                sent(1, 2, p, c, me + PLANE)
            sent(4, 1, p, c, base + px)
            sent(5, 1, p, c, base + py)
            sent(6, 1, px, c, base + py)

        @pl.when(z >= y_from)
        def _():
            sent(7, y_from, py, c, base + px)
    each(drain)

    @pl.when(me == 0)
    def _():
        sink_copy(0, sink, base + px).wait_send()

    @pl.when(me <= 1)
    def _():
        sink_copy(1, sink, base + py).wait_send()

    @pl.when(z + 1 < n_z)
    def _():
        sink_copy(2, sink, me + PLANE).wait_send()

    def gone(t, carry):
        for step in range(1, n_head):
            give(t, step).wait_send()
        return carry
    lax.fori_loop(0, tiles, gone, 0)


def shards(n_seq, n_head, queries, key_rows, value_rows, windows, sink_counts, sink_bias, out_weight):
    rows, heads, width = queries.shape
    kv_heads = key_rows.shape[1]
    group = heads // kv_heads
    lanes = group * rows
    depth, model = out_weight.shape
    assert (WINDOW - 1) // rows + 1 == 2 * PLANE and n_seq % PLANE == 0
    keys, values = key_rows.transpose(1, 0, 2), value_rows.transpose(1, 0, 2)
    q = queries.transpose(1, 0, 2).reshape(kv_heads, lanes, width)
    tile = min(512, model)
    tiles = model // tile
    share = rows // n_head
    bf16, f32, i32 = jnp.bfloat16, jnp.float32, jnp.int32
    vmem = pl.BlockSpec(memory_space=pltpu.VMEM)
    smem = pl.BlockSpec(memory_space=pltpu.SMEM)
    dma = pltpu.SemaphoreType.DMA
    return pl.pallas_call(
        functools.partial(kernel, n_seq, n_head, tile),
        out_shape=jax.ShapeDtypeStruct((share, model), bf16),
        in_specs=[smem, smem, smem] + [pl.BlockSpec(memory_space=pl.ANY)] * 4,
        out_specs=vmem,
        scratch_shapes=[
            pltpu.VMEM((kv_heads, 2, rows, width), bf16),
            pltpu.VMEM((kv_heads, lanes, width), bf16),
            pltpu.VMEM((3 * PLANE, kv_heads, 2, rows, width), bf16),
            pltpu.VMEM((kv_heads, 2, SINK_ROWS, width), bf16),
            pltpu.VMEM((kv_heads, width, lanes), bf16),
            pltpu.VMEM((kv_heads, 1, lanes), i32),
            pltpu.VMEM((kv_heads, 1, lanes), i32),
            pltpu.VMEM((kv_heads, 1, lanes), f32),
            pltpu.VMEM((kv_heads, 1, lanes), f32),
            pltpu.VMEM((kv_heads, 1, lanes), f32),
            pltpu.VMEM((kv_heads, width, lanes), f32),
            pltpu.VMEM((rows, depth), bf16),
            pltpu.VMEM((depth, model), bf16),
            pltpu.VMEM((tiles, n_head, share, tile), bf16),
            pltpu.VMEM((tiles, n_head - 1, share, tile), bf16),
            dma((8, kv_heads)),
            dma((3 * PLANE, kv_heads)),
            dma((3,)),
            dma,
            dma((kv_heads, 2)),
            dma,
            dma,
            dma((tiles, n_head - 1)),
            dma((tiles, n_head - 1)),
        ],
        compiler_params=pltpu.CompilerParams(
            collective_id=0, has_side_effects=True, vmem_limit_bytes=56 * 1024 * 1024
        ),
    )(windows, sink_counts, sink_bias, keys, values, q, out_weight)


def solution(mesh):
    in_specs = (
        P("seq", "head", None),
        P("seq", "head", None),
        P("seq", "head", None),
        P("head"),
        P("head"),
        P("head"),
        P("head", None),
    )
    body = functools.partial(shards, mesh.shape["seq"], mesh.shape["head"])
    out_specs = P(("seq", "head"), None)
    return jax.shard_map(body, mesh=mesh, in_specs=in_specs, out_specs=out_specs, check_vma=False)
```
